32 devices in a mesh: ta: 16 (over z, y, x), gz: 2 (over core).
Axes of the slice: x: 2, y: 2, z: 4, core: 2. Of those that a mesh axis runs over, the one named last changes fastest.
Arguments:
- propagator: float32 [2, 12, 12, 16, 13824], P(None, None, None, 'ta', 'gz'), may hold values from -6 to 6
- backward: float32 [2, 12, 12, 16, 13824], P(None, None, None, 'ta', 'gz'), may hold values from -6 to 6
- sink_time: int32 [1], replicated, may hold values from 0 to 15
- source_position: int32 [3], replicated, may hold values from 0 to 23
- momenta: int32 [27, 3], replicated, may hold values from -3 to 3
- gamma_table: int32 [16], replicated, may hold values from 0 to 15, each once
Outputs:
- correlator: float32 [2, 16, 16, 27], P(None, 'ta', 'gz')
The draws below stay inside these ranges and needn't reach their ends.
Inputs may be any that keep to these rules, and one draw needn't show every extreme that they name: `gamma_table`: each of 0 to 15 appears exactly once.
All inputs are finite; a program needn't handle non-finite values.
Results may differ from the reference program's by a relative error of at most 0.00007.
Values sent between devices are 32-bit elements; how exact they have to be, the bound alone decides.
A program may use at most 192 MiB of HBM per device.

```python
import math
import jax
import jax.numpy as jnp
import numpy as np
from jax import lax

L = 24
NG = 16
NP = 27
T_SIZE = 16
V3 = 13824


def place_ends(drawn, stream_key, smallest, largest):
    shape = drawn.shape
    place = [jax.random.randint(jax.random.fold_in(stream_key, axis), (), 0, shape[axis]) for axis in range(len(shape))]
    drawn = drawn.at[tuple(place)].set(smallest)
    longest = shape.index(max(shape))
    place[longest] = (place[longest] + 1) % shape[longest]
    return drawn.at[tuple(place)].set(largest)


def steps_of(rng, extent, cuts, low, top_value):
    loudness, own = 1.0, jax.random.fold_in(rng, 6)
    for position, shards_of in cuts:
        heights = jnp.exp(jax.random.uniform(jax.random.fold_in(own, position), (shards_of,), jnp.float32, low / len(cuts), top_value / len(cuts)))
        loudness = loudness * jnp.repeat(heights, extent[position] // shards_of).reshape([-1 if axis == position else 1 for axis in range(len(extent))])
    return loudness


def scatter_about(own_key, shape, scale, most, shards=(), kind=jnp.bfloat16):
    gain = steps_of(own_key, shape, shards, -0.22, 0.18) if shards else 1.0
    values = jax.random.normal(own_key, shape, jnp.float32) * scale * gain
    return jnp.minimum(jnp.maximum(values, -most), most).astype(kind)


def setup_inputs(seed: int = 0) -> dict:
    seeds = jax.random.split(jax.random.key(seed), 7)
    return {
        "propagator": scatter_about(seeds[0], (2, 12, 12, T_SIZE, V3), 1.0, 6.0, ((3, 16), (4, 2)), jnp.float32),
        "backward": scatter_about(seeds[1], (2, 12, 12, T_SIZE, V3), 1.0, 6.0, ((3, 16), (4, 2)), jnp.float32),
        "sink_time": jax.random.randint(seeds[2], (1,), 0, T_SIZE).astype(jnp.int32),
        "source_position": jax.random.randint(seeds[3], (3,), 0, L).astype(jnp.int32),
        "momenta": place_ends(jax.random.randint(seeds[4], (NP, 3), -3, 4), jax.random.fold_in(seeds[4], 1), -3, 3).astype(jnp.int32),
        "gamma_table": jax.random.permutation(seeds[5], NG).astype(jnp.int32),
    }


def gamma_tables():
    paulis = [np.eye(2), np.array([[0.0, 1.0], [1.0, 0.0]]), np.array([[0.0, -1j], [1j, 0.0]]), np.array([[1.0, 0.0], [0.0, -1.0]])]
    matrices = np.stack([np.kron(paulis[number // 4], paulis[number % 4]) for number in range(16)])
    return np.stack([matrices.real, matrices.imag]).astype(np.float32)

def complex_product(einsum_form, left_term, right_term):

    def product(first_op, second_op):
        return jnp.einsum(einsum_form, first_op, second_op, precision=lax.Precision.HIGHEST)
    real_part = product(left_term[0], right_term[0]) - product(left_term[1], right_term[1])
    imag_part = product(left_term[0], right_term[1]) + product(left_term[1], right_term[0])
    return jnp.stack([real_part, imag_part])

def complex_reduce(left_term, right_term, reduce_axis):
    real_part = lax.optimization_barrier(jnp.sum(left_term[0] * right_term[0] - left_term[1] * right_term[1], axis=reduce_axis))
    imag_part = lax.optimization_barrier(jnp.sum(left_term[0] * right_term[1] + left_term[1] * right_term[0], axis=reduce_axis))
    return jnp.stack([real_part, imag_part])

def conjugate(values):
    return jnp.stack([values[0], -values[1]])

def source_field(sink_slice):
    return 0.125 * complex_reduce(sink_slice[:, :, None, :, :], sink_slice[:, None, :, :, :], 2)

def phase_table(site_index, source_position, momenta):
    zplane = site_index // (L * L)
    xline = site_index // L % L
    yline = site_index % L
    wave = momenta[:, 0:1] * (xline[None, :] - source_position[0]) + momenta[:, 1:2] * (yline[None, :] - source_position[1]) + momenta[:, 2:3] * (zplane[None, :] - source_position[2])
    wave = jnp.mod(wave, L)
    angle_value = wave.astype(jnp.float32) * (2.0 * math.pi / L)
    return jnp.stack([jnp.cos(angle_value), -jnp.sin(angle_value)])

def slice_correlator(forward, back_field, sink_field, phases, gammas):
    site_count = forward.shape[-1]
    bound = complex_reduce(back_field[:, :, :, None, :], sink_field[:, None, :, :, :], 1)
    forward_split = forward.reshape(2, 4, 36, site_count)
    bound_split = conjugate(bound).reshape(2, 4, 36, site_count)
    spin_block = complex_reduce(forward_split[:, :, None, :, :], bound_split[:, None, :, :, :], 2)
    gamma_flat = jnp.transpose(gammas, (0, 1, 3, 2)).reshape(2, 16, 16)
    currents = complex_product('gb,bs->gs', gamma_flat, spin_block.reshape(2, 16, site_count))
    scale_factor = 1.0 / (72.0 * math.sqrt(L * L * L))
    return scale_factor * complex_product('gs,ps->gp', currents, phases)

def select_currents(gamma_table, values):
    onehot = (gamma_table[:, None] == jnp.arange(NG, dtype=jnp.int32)[None, :]).astype(jnp.float32)
    return jnp.einsum('cg,xgp->xcp', onehot, values, precision=lax.Precision.HIGHEST)

def reference(propagator, backward, sink_time, source_position, momenta, gamma_table):
    gammas = jnp.asarray(gamma_tables())
    sink_slice = lax.dynamic_index_in_dim(propagator, sink_time[0], 3, keepdims=False)
    sink_field = source_field(sink_slice)
    phases = phase_table(jnp.arange(L * L * L, dtype=jnp.int32), source_position, momenta)

    def one_slice(slice_index):
        forward = lax.dynamic_index_in_dim(propagator, slice_index, 3, keepdims=False)
        back_field = lax.dynamic_index_in_dim(backward, slice_index, 3, keepdims=False)
        return select_currents(gamma_table, slice_correlator(forward, back_field, sink_field, phases, gammas))
    stacked = lax.map(one_slice, jnp.arange(T_SIZE, dtype=jnp.int32))
    return jnp.transpose(stacked, (1, 0, 2, 3))
```

```python
import math
import random

import jax
import jax.numpy as jnp
import numpy as np
from jax import lax
from jax.experimental import pallas as pl
from jax.experimental.pallas import tpu as pltpu
from jax.sharding import PartitionSpec as P

L = 24
NG = 16
LANES = 128
SUB = 8
SPINCOLOR = 12
COMPS = 2 * SPINCOLOR * SPINCOLOR
PAIRS = [(row, column) for row in range(SPINCOLOR) for column in range(row, SPINCOLOR)]
PAIR_NUMBER = {pair: number for number, pair in enumerate(PAIRS)}
HOP_SLOTS = 6
MESH = pl.DeviceIdType.MESH
HIGHEST = lax.Precision.HIGHEST


def gamma_tables():
    paulis = [
        np.eye(2),
        np.array([[0.0, 1.0], [1.0, 0.0]]),
        np.array([[0.0, -1j], [1j, 0.0]]),
        np.array([[1.0, 0.0], [0.0, -1.0]]),
    ]
    matrices = np.stack([np.kron(paulis[number // 4], paulis[number % 4]) for number in range(16)])
    return np.stack([matrices.real, matrices.imag]).astype(np.float32)


class Grid:
    def __init__(self, mesh):
        devices = mesh.devices.reshape(mesh.shape["ta"], -1)[:, 0]
        self.nodes = len(devices)
        self.dims, self.strides, self.wrap = [self.nodes], [1], False
        coords = [getattr(device, "coords", None) for device in devices]
        if all(coord is not None for coord in coords):
            self.read(np.array([list(coord) for coord in coords]))
        self.dirs = []
        for axis, size in enumerate(self.dims):
            if size == 2:
                self.dirs.append((axis, 0))
            elif size > 2:
                self.dirs += [(axis, 1), (axis, -1)]

    def read(self, coords):
        coords = coords - coords.min(axis=0)
        sizes = coords.max(axis=0) + 1
        found = []
        for axis in range(coords.shape[1]):
            if sizes[axis] > 1:
                unit = np.zeros(coords.shape[1], int)
                unit[axis] = 1
                hits = np.flatnonzero((coords == unit).all(axis=1))
                if len(hits) != 1:
                    return
                found.append((int(hits[0]), int(sizes[axis]), axis))
        found.sort(reverse=True)
        index = np.arange(self.nodes)
        for stride, size, axis in found:
            if ((index // stride) % size != coords[:, axis]).any():
                return
        if math.prod(size for _, size, _ in found) != self.nodes:
            return
        self.dims = [size for _, size, _ in found]
        self.strides = [stride for stride, _, _ in found]
        self.wrap = len(found) == 3 and all(size % 4 == 0 for size in self.dims)

    def position(self, node):
        return [node // stride % size for stride, size in zip(self.strides, self.dims)]

    def node(self, position):
        return sum(c * stride for c, stride in zip(position, self.strides))

    def step(self, node, number):
        axis, sign = self.dirs[number]
        place = self.position(node)
        place[axis] = 1 - place[axis] if sign == 0 else place[axis] + sign
        if self.wrap:
            place[axis] %= self.dims[axis]
        if not 0 <= place[axis] < self.dims[axis]:
            return None
        return self.node(place)


def grow(edges, nodes, root, count, rng, deepest):
    used = set()
    depth = [{root: 0} for _ in range(count)]
    parent = [{} for _ in range(count)]
    from_root = [0] * count
    for _ in range(deepest):
        options = [
            (k, u, d, v)
            for k in range(count)
            for u in depth[k]
            for d, v in edges[u]
            if v not in depth[k] and (u, d) not in used
        ]
        rng.shuffle(options)
        ways = {}
        for k, _, _, v in options:
            ways[k, v] = ways.get((k, v), 0) + 1
        options.sort(key=lambda option: ways[option[0], option[3]] + 1.5 * rng.random())
        level = [{} for _ in range(count)]
        taken = [0] * count
        for k, u, d, v in options:
            if v in depth[k] or v in level[k] or (u, d) in used:
                continue
            if u == root:
                if taken[k] or (from_root[k] and rng.random() < 0.7):
                    continue
                taken[k] = 1
                from_root[k] += 1
            level[k][v] = depth[k][u] + 1
            parent[k][v] = (u, d)
            used.add((u, d))
        for k in range(count):
            depth[k].update(level[k])
        if all(len(known) == nodes for known in depth):
            return sorted(max(known.values()) for known in depth)[::-1], parent, depth
    return None


def route(grid, root):
    edges = {
        u: [
            (d, v)
            for d in range(len(grid.dirs))
            for v in [grid.step(u, d)]
            if v is not None and v != u
        ]
        for u in range(grid.nodes)
    }
    rng = random.Random(7)
    most = min(3, min(len(links) for links in edges.values()))
    for count in range(most, 0, -1):
        best = None
        for _ in range(400 if grid.nodes <= 16 else 40):
            found = grow(edges, grid.nodes, root, count, rng, 2 * sum(grid.dims))
            if found and (best is None or found[0] < best[0]):
                best = found
        if best:
            return count, best[1], best[2]
    raise ValueError("no route")


def routes(grid):
    plans = {}
    for root in range(grid.nodes):
        place = grid.position(root)
        if grid.wrap:
            canonical = 0
        else:
            canonical = grid.node([min(c, n - 1 - c) for c, n in zip(place, grid.dims)])
        if canonical not in plans:
            plans[canonical] = route(grid, canonical)
    trees = min(plan[0] for plan in plans.values())
    width = 1 + 2 * trees + len(grid.dirs)
    table = np.full((grid.nodes, grid.nodes, width), -1, np.int32)
    deepest = 0
    for root in range(grid.nodes):
        place = grid.position(root)
        if grid.wrap:
            canonical, flips = 0, [False] * len(place)
        else:
            flips = [c > n - 1 - c for c, n in zip(place, grid.dims)]
            canonical = grid.node([min(c, n - 1 - c) for c, n in zip(place, grid.dims)])

        def image(node):
            there = grid.position(node)
            if grid.wrap:
                return grid.node([(c + o) % n for c, o, n in zip(there, place, grid.dims)])
            return grid.node([n - 1 - c if f else c for c, f, n in zip(there, flips, grid.dims)])

        def turned(d):
            axis, sign = grid.dirs[d]
            return grid.dirs.index((axis, -sign if flips[axis] else sign))

        _, parent, depth = plans[canonical]
        for k in range(trees):
            for v in range(grid.nodes):
                row = table[image(v), root]
                row[0] = v == canonical
                row[1 + trees + k] = depth[k][v]
                deepest = max(deepest, depth[k][v])
                if v != canonical:
                    u, d = parent[k][v]
                    row[1 + k] = turned(d)
                    sender = table[image(u), root]
                    assert sender[1 + 2 * trees + turned(d)] == -1
                    sender[1 + 2 * trees + turned(d)] = k
    return trees, deepest, table


def multiply_add(total, left, right):
    real = left[0] * right[0] - left[1] * right[1]
    imag = left[0] * right[1] + left[1] * right[0]
    return (real, imag) if total is None else (total[0] + real, total[1] + imag)


def multiply_add_conj(total, left, right):
    real = left[0] * right[0] + left[1] * right[1]
    imag = left[1] * right[0] - left[0] * right[1]
    return (real, imag) if total is None else (total[0] + real, total[1] + imag)


def make_kernel(grid, trees, deepest, rows, momentum_count, currents):
    blocks = pl.cdiv(rows, SUB)
    piece = blocks
    share = 2 * len(PAIRS) // trees
    slots = share * blocks // piece
    hop = HOP_SLOTS
    ring = 2 * hop
    directions = len(grid.dirs)
    all_slots = slots + hop * deepest
    sends = all_slots - hop
    half = SPINCOLOR * SPINCOLOR * rows
    span = half + (SPINCOLOR - 1) * rows + SUB
    sigma_units = 6
    spin_units = SPINCOLOR
    piece_rows = piece * SUB
    padded = 32

    def kernel(
        sink_ref, source_ref, gamma_ref, momenta_ref, mix_ref, table_ref, s_hbm, h_hbm,
        out_ref,
        s_ref, h_ref, own_ref, a_ref, tree_ref, in_ref, stage_ref, phase_ref, m_ref, acc_ref, w_ref,
        send_ref, got_ref, plan_ref,
        load_sem, plan_sem, send_sem, recv_sem, pair_sem,
    ):
        me = lax.axis_index("ta")
        core = lax.axis_index("gz")
        partner = 1 - core
        total_rows = COMPS * rows
        load_s = pltpu.make_async_copy(s_hbm, s_ref.at[pl.ds(0, total_rows)], load_sem.at[0])
        load_h = pltpu.make_async_copy(h_hbm, h_ref.at[pl.ds(0, total_rows)], load_sem.at[1])
        load_s.start()
        load_plan = pltpu.make_async_copy(table_ref.at[me], plan_ref, plan_sem)
        load_plan.start()

        neighbours, has_out, has_in = [], [], []
        for axis, sign in grid.dirs:
            stride, size = grid.strides[axis], grid.dims[axis]
            place = me // stride % size
            if sign == 0:
                neighbours.append(me + stride * (1 - 2 * place))
                has_out.append(None)
                has_in.append(None)
            elif grid.wrap:
                neighbours.append(me + stride * ((place + sign + size) % size - place))
                has_out.append(None)
                has_in.append(None)
            else:
                neighbours.append(me + stride * sign)
                has_out.append(place < size - 1 if sign > 0 else place > 0)
                has_in.append(place > 0 if sign > 0 else place < size - 1)

        def when(condition, action):
            if condition is None:
                action()
            else:
                pl.when(condition)(action)

        barrier = pltpu.get_barrier_semaphore()
        pl.semaphore_signal(barrier, 1, device_id={"gz": partner}, device_id_type=MESH)
        for d in range(directions):

            def greet(d=d):
                pl.semaphore_signal(
                    barrier, 1, device_id={"ta": neighbours[d]}, device_id_type=MESH
                )

            when(has_out[d], greet)

        acc_ref[...] = jnp.zeros_like(acc_ref)
        s_ref[pl.ds(total_rows, SUB)] = jnp.zeros((SUB, LANES), jnp.float32)
        h_ref[pl.ds(total_rows, SUB)] = jnp.zeros((SUB, LANES), jnp.float32)
        names = lax.broadcasted_iota(jnp.int32, (1, NG), 1)
        onehot = jnp.concatenate(
            [
                jnp.where(names == jnp.full((1, NG), gamma_ref[core * currents + c]), 1.0, 0.0)
                for c in range(currents)
            ],
            axis=0,
        )
        for part in range(2):
            w_ref[part * currents : (part + 1) * currents] = lax.dot_general(
                onehot,
                mix_ref[part],
                (((1,), (0,)), ((), ())),
                precision=HIGHEST,
                preferred_element_type=jnp.float32,
            )
        momenta = momenta_ref[...].astype(jnp.float32)
        momenta = jnp.concatenate(
            [momenta, jnp.zeros((padded - momentum_count, 3), jnp.float32)], axis=0
        )
        source = [source_ref[i].astype(jnp.float32) for i in range(3)]

        load_plan.wait()
        sink = sink_ref[0]
        width = 1 + 2 * trees + directions

        def pick(candidate, chosen):
            return tuple(
                jnp.where(sink == candidate, plan_ref[0, candidate * width + q], chosen[q])
                for q in range(width)
            )

        plan = lax.fori_loop(0, grid.nodes, pick, (jnp.int32(-1),) * width)
        everywhere = [jnp.full((SUB, LANES), value, jnp.int32) for value in plan]
        is_source = everywhere[0] == 1
        parents = everywhere[1 : 1 + trees]
        depths = everywhere[1 + trees : 1 + 2 * trees]
        loads = everywhere[1 + 2 * trees :]

        def run(unit, start, stop):
            lax.fori_loop(start, stop, lambda u, carry: (unit(u), carry)[1], 0)

        def sigma_unit(unit):
            block, r = unit // sigma_units, unit % sigma_units
            base = block * SUB
            for i in range(SPINCOLOR + 1):
                first = i < SPINCOLOR - r
                row = jnp.where(first, r, SPINCOLOR - 1 - r)
                column = jnp.where(first, r + i, i - 1)
                total = None
                a = s_ref.at[pl.ds(row * (SPINCOLOR * rows) + base, span)]
                b = s_ref.at[pl.ds(column * (SPINCOLOR * rows) + base, span)]
                for m in range(SPINCOLOR):
                    left = (a[pl.ds(m * rows, SUB)], a[pl.ds(half + m * rows, SUB)])
                    right = (b[pl.ds(m * rows, SUB)], b[pl.ds(half + m * rows, SUB)])
                    total = multiply_add(total, left, right)
                number = row * SPINCOLOR - (row * (row - 1)) // 2 + column - row
                tree = number // (share // 2)
                place = (
                    tree * (share * blocks)
                    + block * share
                    + 2 * (number - tree * (share // 2))
                ) * SUB
                place = pl.multiple_of(place, SUB)
                own_ref[pl.ds(place, SUB)] = 0.125 * total[0]
                own_ref[pl.ds(place + SUB, SUB)] = 0.125 * total[1]

        def phase_row(number):
            lane = lax.broadcasted_iota(jnp.int32, (1, LANES), 1)
            site = (core * (rows * LANES) + number * LANES + lane).astype(jnp.float32)
            zplane = jnp.floor((site + 0.5) * (1.0 / (L * L)))
            rest = site - zplane * (L * L)
            xline = jnp.floor((rest + 0.5) * (1.0 / L))
            yline = rest - xline * L
            wave = (
                momenta[:, 0:1] * (xline - source[0])
                + momenta[:, 1:2] * (yline - source[1])
                + momenta[:, 2:3] * (zplane - source[2])
            )
            wave = wave - L * jnp.floor((wave + 0.5) * (1.0 / L)) - L / 2
            x = wave * (math.pi / L)
            y = x * x
            s = x * (1 + y * (-1 / 6 + y * (1 / 120 + y * (-1 / 5040 + y * (1 / 362880 - y / 39916800)))))
            c = 1 + y * (
                -1 / 2
                + y * (1 / 24 + y * (-1 / 720 + y * (1 / 40320 + y * (-1 / 3628800 + y / 479001600))))
            )
            inside = jnp.where(number < rows, 1.0, 0.0)
            block = number // SUB
            lanes = pl.ds(pl.multiple_of(number % SUB * LANES, LANES), LANES)
            phase_ref[block, 0:padded, lanes] = (2.0 * s * s - 1.0) * inside
            phase_ref[block, padded : 2 * padded, lanes] = (2.0 * s * c) * inside

        def spin_unit(unit):
            block, r = unit // spin_units, unit % spin_units
            alpha, color = r // 3, r % 3
            h = h_ref.at[pl.ds(r * (SPINCOLOR * rows) + block * SUB, span)]
            s = s_ref.at[
                pl.ds(color * (SPINCOLOR * rows) + block * SUB, span + 9 * SPINCOLOR * rows)
            ]
            sigma = [
                tree_ref.at[k, pl.ds(pl.multiple_of(block * (share * SUB), SUB), share * SUB)]
                for k in range(trees)
            ]

            def sigma_at(row, column):
                number = PAIR_NUMBER[min(row, column), max(row, column)]
                tree, place = number // (share // 2), number % (share // 2) * 2 * SUB
                return sigma[tree][place : place + SUB], sigma[tree][place + SUB : place + 2 * SUB]

            h_row = [(h[pl.ds(m * rows, SUB)], h[pl.ds(half + m * rows, SUB)]) for m in range(SPINCOLOR)]
            sums = [None] * 4
            for k in range(SPINCOLOR):
                total = None
                for m in range(SPINCOLOR):
                    total = multiply_add(total, h_row[m], sigma_at(m, k))
                for beta in range(4):
                    start = (beta * 3 * SPINCOLOR + k) * rows
                    forward = (s[pl.ds(start, SUB)], s[pl.ds(half + start, SUB)])
                    sums[beta] = multiply_add_conj(sums[beta], forward, total)
            for beta in range(4):
                for part in range(2):
                    place = pl.ds(pl.multiple_of((part * 16 + beta * 4 + alpha) * SUB, SUB), SUB)
                    m_ref[place] = sums[beta][part] + jnp.where(color > 0, m_ref[place], 0.0)

            @pl.when(r == spin_units - 1)
            def _():
                spin = jnp.concatenate(
                    [m_ref[pl.ds(i, 32, stride=SUB), :] for i in range(SUB)], axis=1
                )
                acc_ref[...] += lax.dot_general(
                    spin,
                    phase_ref[block],
                    (((1,), (1,)), ((), ())),
                    precision=HIGHEST,
                    preferred_element_type=jnp.float32,
                )

        def out_copy(d, slot):
            place = slot % ring
            return pltpu.make_async_remote_copy(
                src_ref=stage_ref.at[d, place],
                dst_ref=in_ref.at[d, place],
                send_sem=send_sem.at[d, place],
                recv_sem=recv_sem.at[d, place],
                device_id={"ta": neighbours[d]},
                device_id_type=MESH,
            )

        def settle(chunk):
            for k in range(trees):
                at_depth = [depths[k] == n for n in range(deepest + 1)]
                for i in range(piece):
                    value = None
                    for n in range(deepest + 1):
                        start = ((chunk + hop * n) * piece + i) * SUB
                        found = a_ref[k, pl.ds(pl.multiple_of(start, SUB), SUB)]
                        value = found if value is None else jnp.where(at_depth[n], found, value)
                    start = pl.multiple_of((chunk * piece + i) * SUB, SUB)
                    tree_ref[k, pl.ds(start, SUB)] = value

        def relay(j):
            @pl.when(j >= hop)
            def _():
                for d in range(directions):
                    when(has_in[d], lambda d=d: out_copy(d, j + hop).wait_recv())

            @pl.when(jnp.logical_and(j >= ring, j < sends + ring))
            def _():
                for d in range(directions):
                    when(has_out[d], lambda d=d: out_copy(d, j).wait_send())

            place = j % ring
            from_place = (j + hop) % ring
            mine = jnp.minimum(j, slots - 1) * piece_rows
            for i in range(piece):
                at = slice(i * SUB, (i + 1) * SUB)
                arrived = [in_ref[d, from_place, at] for d in range(directions)]
                values = []
                for k in range(trees):
                    value = arrived[0]
                    for d in range(1, directions):
                        value = jnp.where(parents[k] == d, arrived[d], value)
                    start = pl.multiple_of(k * (share * blocks * SUB) + mine + i * SUB, SUB)
                    value = jnp.where(is_source, own_ref[pl.ds(start, SUB)], value)
                    a_ref[k, pl.ds(pl.multiple_of(j * piece_rows + i * SUB, SUB), SUB)] = value
                    values.append(value)
                for d in range(directions):
                    value = values[0]
                    for k in range(1, trees):
                        value = jnp.where(loads[d] == k, values[k], value)
                    stage_ref[d, place, at] = value

            @pl.when(j >= hop * deepest)
            def _():
                settle(j - hop * deepest)

            @pl.when(j < sends)
            def _():
                for d in range(directions):
                    when(has_out[d], lambda d=d: out_copy(d, j).start())

        load_s.wait()
        load_h.start()
        run(sigma_unit, 0, sigma_units)

        peers = 1
        for known in has_in:
            peers += 1 if known is None else known.astype(jnp.int32)
        pl.semaphore_wait(barrier, peers)

        def sigma_until(j):
            done = sigma_units + (sigma_units * (blocks * (j + 2)) + slots - 1) // slots
            return jnp.where(j < 0, sigma_units, jnp.minimum(done, sigma_units * blocks))

        phase_count = blocks * SUB

        first = hop * deepest + (share - 1) // piece
        spin_total = spin_units * blocks

        def spin_until(j):
            done = (j - first) * spin_total // slots + 1
            return jnp.where(j < first, 0, jnp.minimum(done, spin_total))

        def step(j, carry):
            relay(j)
            run(sigma_unit, sigma_until(j - 1), sigma_until(j))
            run(
                phase_row,
                jnp.minimum(2 * j, phase_count),
                jnp.minimum(2 * j + 2, phase_count),
            )

            @pl.when(j == first)
            def _():
                load_h.wait()

            run(spin_unit, spin_until(j - 1), spin_until(j))
            return carry

        lax.fori_loop(0, all_slots, step, 0)
        run(spin_unit, spin_until(jnp.int32(all_slots - 1)), spin_total)
        for slot in range(all_slots - ring, sends):
            for d in range(directions):
                when(has_out[d], lambda d=d, slot=slot: out_copy(d, slot).wait_send())

        real = acc_ref[0:16, 0:padded] - acc_ref[16:32, padded : 2 * padded]
        imag = acc_ref[0:16, padded : 2 * padded] + acc_ref[16:32, 0:padded]
        send_ref[0:16, 0:padded] = real
        send_ref[16:32, 0:padded] = imag
        swap = pltpu.make_async_remote_copy(
            src_ref=send_ref,
            dst_ref=got_ref,
            send_sem=pair_sem.at[0],
            recv_sem=pair_sem.at[1],
            device_id={"gz": partner},
            device_id_type=MESH,
        )
        swap.start()
        swap.wait()
        both = send_ref[:, 0:padded] + got_ref[:, 0:padded]
        result = lax.dot_general(
            w_ref[...],
            both,
            (((1,), (0,)), ((), ())),
            precision=HIGHEST,
            preferred_element_type=jnp.float32,
        )
        out_ref[0, 0] = result[0:currents, 0:momentum_count]
        out_ref[1, 0] = result[currents : 2 * currents, 0:momentum_count]

    scratch = [
        pltpu.VMEM((COMPS * rows + SUB, LANES), jnp.float32),
        pltpu.VMEM((COMPS * rows + SUB, LANES), jnp.float32),
        pltpu.VMEM((trees * share * blocks * SUB, LANES), jnp.float32),
        pltpu.VMEM((trees, all_slots * piece_rows, LANES), jnp.float32),
        pltpu.VMEM((trees, share * blocks * SUB, LANES), jnp.float32),
        pltpu.VMEM((directions, ring, piece_rows, LANES), jnp.float32),
        pltpu.VMEM((directions, ring, piece_rows, LANES), jnp.float32),
        pltpu.VMEM((blocks, 2 * padded, SUB * LANES), jnp.float32),
        pltpu.VMEM((32 * SUB, LANES), jnp.float32),
        pltpu.VMEM((32, 2 * padded), jnp.float32),
        pltpu.VMEM((2 * currents, 32), jnp.float32),
        pltpu.VMEM((32, LANES), jnp.float32),
        pltpu.VMEM((32, LANES), jnp.float32),
        pltpu.SMEM((1, plan_width(grid, trees)), jnp.int32),
        pltpu.SemaphoreType.DMA((2,)),
        pltpu.SemaphoreType.DMA(()),
        pltpu.SemaphoreType.DMA((directions, ring)),
        pltpu.SemaphoreType.DMA((directions, ring)),
        pltpu.SemaphoreType.DMA((2,)),
    ]
    return kernel, scratch


def plan_width(grid, trees):
    used = grid.nodes * (1 + 2 * trees + len(grid.dirs))
    return pl.cdiv(used, LANES) * LANES


def mixing():
    real, imag = np.transpose(gamma_tables(), (0, 1, 3, 2)).reshape(2, 16, 16)
    scale = 1.0 / (72.0 * math.sqrt(L * L * L))
    return (
        scale
        * np.stack([np.concatenate([real, -imag], axis=1), np.concatenate([imag, real], axis=1)])
    ).astype(np.float32)


def solution(mesh):
    grid = Grid(mesh)
    trees, deepest, table = routes(grid)
    cores = mesh.shape["gz"]
    width = plan_width(grid, trees)
    flat = table.reshape(grid.nodes, -1)
    plans = np.zeros((grid.nodes, 1, width), np.int32)
    plans[:, 0, : flat.shape[1]] = flat
    mix = mixing()

    def body(propagator, backward, sink_time, source_position, momenta, gamma_table):
        local_times, site_count = propagator.shape[3:]
        assert local_times == 1 and cores == 2 and site_count % LANES == 0
        rows = site_count // LANES
        momentum_count = momenta.shape[0]
        currents = gamma_table.shape[0] // cores
        kernel, scratch = make_kernel(grid, trees, deepest, rows, momentum_count, currents)
        vmem, smem = (
            pl.BlockSpec(memory_space=pltpu.VMEM),
            pl.BlockSpec(memory_space=pltpu.SMEM),
        )
        anywhere = pl.BlockSpec(memory_space=pl.ANY)
        return pl.pallas_call(
            kernel,
            out_shape=jax.ShapeDtypeStruct((2, 1, currents, momentum_count), jnp.float32),
            in_specs=[smem, smem, smem, vmem, vmem, anywhere, anywhere, anywhere],
            out_specs=vmem,
            scratch_shapes=scratch,
            compiler_params=pltpu.CompilerParams(
                collective_id=0, has_side_effects=True, vmem_limit_bytes=60 << 20
            ),
            name="three_point",
        )(
            sink_time,
            source_position,
            gamma_table,
            momenta,
            jnp.asarray(mix),
            jnp.asarray(plans),
            propagator.reshape(COMPS * rows, LANES),
            backward.reshape(COMPS * rows, LANES),
        )

    in_specs = (
        P(None, None, None, "ta", "gz"),
        P(None, None, None, "ta", "gz"),
        P(),
        P(),
        P(),
        P(),
    )
    out_specs = P(None, "ta", "gz", None)
    return jax.shard_map(body, mesh=mesh, in_specs=in_specs, out_specs=out_specs, check_vma=False)
```

```python
import math
import random

import jax
import jax.numpy as jnp
import numpy as np
from jax import lax
from jax.experimental import pallas as pl
from jax.experimental.pallas import tpu as pltpu
from jax.sharding import PartitionSpec as P

L = 24
NG = 16
LANES = 128
SUB = 8
SPINCOLOR = 12
PAIRS = [(row, column) for row in range(SPINCOLOR) for column in range(row, SPINCOLOR)]
PAIR_NUMBER = {pair: number for number, pair in enumerate(PAIRS)}
HOP_SLOTS = (6, 4)
PIECE = 7
MESH = pl.DeviceIdType.MESH
HIGHEST = lax.Precision.HIGHEST


def gamma_tables():
    paulis = [
        np.eye(2),
        np.array([[0.0, 1.0], [1.0, 0.0]]),
        np.array([[0.0, -1j], [1j, 0.0]]),
        np.array([[1.0, 0.0], [0.0, -1.0]]),
    ]
    matrices = np.stack([np.kron(paulis[number // 4], paulis[number % 4]) for number in range(16)])
    return np.stack([matrices.real, matrices.imag]).astype(np.float32)


class Grid:
    def __init__(self, mesh):
        devices = mesh.devices.reshape(mesh.shape["ta"], -1)[:, 0]
        self.nodes = len(devices)
        self.dims, self.strides, self.wrap = [self.nodes], [1], False
        coords = [getattr(device, "coords", None) for device in devices]
        if all(coord is not None for coord in coords):
            self.read(np.array([list(coord) for coord in coords]))
        self.dirs = []
        for axis, size in enumerate(self.dims):
            if size == 2:
                self.dirs.append((axis, 0))
            elif size > 2:
                self.dirs += [(axis, 1), (axis, -1)]

    def read(self, coords):
        coords = coords - coords.min(axis=0)
        sizes = coords.max(axis=0) + 1
        found = []
        for axis in range(coords.shape[1]):
            if sizes[axis] > 1:
                unit = np.zeros(coords.shape[1], int)
                unit[axis] = 1
                hits = np.flatnonzero((coords == unit).all(axis=1))
                if len(hits) != 1:
                    return
                found.append((int(hits[0]), int(sizes[axis]), axis))
        found.sort(reverse=True)
        index = np.arange(self.nodes)
        for stride, size, axis in found:
            if ((index // stride) % size != coords[:, axis]).any():
                return
        if math.prod(size for _, size, _ in found) != self.nodes:
            return
        self.dims = [size for _, size, _ in found]
        self.strides = [stride for stride, _, _ in found]
        self.wrap = len(found) == 3 and all(size % 4 == 0 for size in self.dims)

    def position(self, node):
        return [node // stride % size for stride, size in zip(self.strides, self.dims)]

    def node(self, position):
        return sum(c * stride for c, stride in zip(position, self.strides))

    def step(self, node, number):
        axis, sign = self.dirs[number]
        place = self.position(node)
        place[axis] = 1 - place[axis] if sign == 0 else place[axis] + sign
        if self.wrap:
            place[axis] %= self.dims[axis]
        if not 0 <= place[axis] < self.dims[axis]:
            return None
        return self.node(place)


def grow(edges, nodes, root, count, rng, deepest):
    used = set()
    depth = [{root: 0} for _ in range(count)]
    parent = [{} for _ in range(count)]
    from_root = [0] * count
    for _ in range(deepest):
        options = [
            (k, u, d, v)
            for k in range(count)
            for u in depth[k]
            for d, v in edges[u]
            if v not in depth[k] and (u, d) not in used
        ]
        rng.shuffle(options)
        ways = {}
        for k, _, _, v in options:
            ways[k, v] = ways.get((k, v), 0) + 1
        options.sort(key=lambda option: ways[option[0], option[3]] + 1.5 * rng.random())
        level = [{} for _ in range(count)]
        taken = [0] * count
        for k, u, d, v in options:
            if v in depth[k] or v in level[k] or (u, d) in used:
                continue
            if u == root:
                if taken[k] or (from_root[k] and rng.random() < 0.7):
                    continue
                taken[k] = 1
                from_root[k] += 1
            level[k][v] = depth[k][u] + 1
            parent[k][v] = (u, d)
            used.add((u, d))
        for k in range(count):
            depth[k].update(level[k])
        if all(len(known) == nodes for known in depth):
            return sorted(max(known.values()) for known in depth)[::-1], parent, depth
    return None


def route(grid, root):
    edges = {
        u: [
            (d, v)
            for d in range(len(grid.dirs))
            for v in [grid.step(u, d)]
            if v is not None and v != u
        ]
        for u in range(grid.nodes)
    }
    rng = random.Random(7)
    most = min(3, min(len(links) for links in edges.values()))
    for count in range(most, 0, -1):
        best = None
        for _ in range(400 if grid.nodes <= 16 else 40):
            found = grow(edges, grid.nodes, root, count, rng, 2 * sum(grid.dims))
            if found and (best is None or found[0] < best[0]):
                best = found
        if best:
            return count, best[1], best[2]
    raise ValueError("no route")


def routes(grid):
    plans = {}
    for root in range(grid.nodes):
        place = grid.position(root)
        if grid.wrap:
            canonical = 0
        else:
            canonical = grid.node([min(c, n - 1 - c) for c, n in zip(place, grid.dims)])
        if canonical not in plans:
            plans[canonical] = route(grid, canonical)
    trees = min(plan[0] for plan in plans.values())
    width = 1 + 2 * trees + len(grid.dirs)
    table = np.full((grid.nodes, grid.nodes, width), -1, np.int32)
    deepest = 0
    for root in range(grid.nodes):
        place = grid.position(root)
        if grid.wrap:
            canonical, flips = 0, [False] * len(place)
        else:
            flips = [c > n - 1 - c for c, n in zip(place, grid.dims)]
            canonical = grid.node([min(c, n - 1 - c) for c, n in zip(place, grid.dims)])

        def image(node):
            there = grid.position(node)
            if grid.wrap:
                return grid.node([(c + o) % n for c, o, n in zip(there, place, grid.dims)])
            return grid.node([n - 1 - c if f else c for c, f, n in zip(there, flips, grid.dims)])

        def turned(d):
            axis, sign = grid.dirs[d]
            return grid.dirs.index((axis, -sign if flips[axis] else sign))

        _, parent, depth = plans[canonical]
        for k in range(trees):
            for v in range(grid.nodes):
                row = table[image(v), root]
                row[0] = v == canonical
                row[1 + trees + k] = depth[k][v]
                deepest = max(deepest, depth[k][v])
                if v != canonical:
                    u, d = parent[k][v]
                    row[1 + k] = turned(d)
                    sender = table[image(u), root]
                    assert sender[1 + 2 * trees + turned(d)] == -1
                    sender[1 + 2 * trees + turned(d)] = k
    return trees, deepest, table


def multiply_add(total, left, right):
    real = left[0] * right[0] - left[1] * right[1]
    imag = left[0] * right[1] + left[1] * right[0]
    return (real, imag) if total is None else (total[0] + real, total[1] + imag)


def multiply_add_conj(total, left, right):
    real = left[0] * right[0] + left[1] * right[1]
    imag = left[1] * right[0] - left[0] * right[1]
    return (real, imag) if total is None else (total[0] + real, total[1] + imag)


def make_kernel(grid, trees, deepest, rows, momentum_count, currents):
    blocks = pl.cdiv(rows, SUB)
    share = 2 * len(PAIRS) // trees
    piece = PIECE if share * blocks % PIECE == 0 else blocks
    slots = share * blocks // piece
    most_hop = max(HOP_SLOTS)
    ring = 2 * most_hop
    directions = len(grid.dirs)
    sigma_units = 6
    spin_units = SPINCOLOR
    piece_rows = piece * SUB
    all_rows = trees * piece_rows
    ready = [
        ((2 * PAIR_NUMBER[k, SPINCOLOR - 1] + 1) // trees + 1) / share for k in range(SPINCOLOR)
    ]
    behind = math.ceil(100 * max(spin_units * ready[k] - k for k in range(SPINCOLOR)))
    padded = 32

    def kernel(
        sink_ref, source_ref, gamma_ref, momenta_ref, mix_ref, table_ref, s_hbm, h_hbm,
        out_ref,
        s_ref, h_ref, hs_ref, own_ref, a_ref, tree_ref, in_ref, stage_ref, phase_ref,
        m_ref, acc_ref, w_ref, send_ref, got_ref, plan_ref,
        load_sem, plan_sem, send_sem, recv_sem, pair_sem,
    ):
        me = lax.axis_index("ta")
        core = lax.axis_index("gz")
        partner = 1 - core
        hop = jnp.where(core == 1, HOP_SLOTS[1], HOP_SLOTS[0])
        all_slots = slots + hop * deepest
        sends = all_slots - hop
        inside = pl.ds(0, rows * LANES)
        load_s = pltpu.make_async_copy(s_hbm, s_ref.at[:, :, :, :, inside], load_sem.at[0])
        load_h = pltpu.make_async_copy(h_hbm, h_ref.at[:, :, :, :, inside], load_sem.at[1])
        load_s.start()
        load_plan = pltpu.make_async_copy(table_ref.at[me], plan_ref, plan_sem)
        load_plan.start()

        neighbours, has_out, has_in = [], [], []
        for axis, sign in grid.dirs:
            stride, size = grid.strides[axis], grid.dims[axis]
            place = me // stride % size
            if sign == 0:
                neighbours.append(me + stride * (1 - 2 * place))
                has_out.append(None)
                has_in.append(None)
            elif grid.wrap:
                neighbours.append(me + stride * ((place + sign + size) % size - place))
                has_out.append(None)
                has_in.append(None)
            else:
                neighbours.append(me + stride * sign)
                has_out.append(place < size - 1 if sign > 0 else place > 0)
                has_in.append(place > 0 if sign > 0 else place < size - 1)

        def when(condition, action):
            if condition is None:
                action()
            else:
                pl.when(condition)(action)

        barrier = pltpu.get_barrier_semaphore()
        pl.semaphore_signal(barrier, 1, device_id={"gz": partner}, device_id_type=MESH)
        for d in range(directions):

            def greet(d=d):
                pl.semaphore_signal(
                    barrier, 1, device_id={"ta": neighbours[d]}, device_id_type=MESH
                )

            when(has_out[d], greet)

        acc_ref[...] = jnp.zeros_like(acc_ref)
        spare = (blocks * SUB - rows) * LANES
        if spare:
            for field in (s_ref, h_ref):
                for part in range(2):
                    for row in range(SPINCOLOR):
                        field[part, row, :, :, pl.ds(rows * LANES, spare)] = jnp.zeros(
                            (SPINCOLOR, 1, spare), jnp.float32
                        )
        names = lax.broadcasted_iota(jnp.int32, (1, NG), 1)
        onehot = jnp.concatenate(
            [
                jnp.where(names == jnp.full((1, NG), gamma_ref[core * currents + c]), 1.0, 0.0)
                for c in range(currents)
            ],
            axis=0,
        )
        for part in range(2):
            w_ref[part * currents : (part + 1) * currents] = lax.dot_general(
                onehot,
                mix_ref[part],
                (((1,), (0,)), ((), ())),
                precision=HIGHEST,
                preferred_element_type=jnp.float32,
            )
        eye = jnp.where(
            lax.broadcasted_iota(jnp.int32, (padded, momentum_count), 0)
            == lax.broadcasted_iota(jnp.int32, (padded, momentum_count), 1),
            1.0,
            0.0,
        )
        momenta = lax.dot_general(
            eye,
            momenta_ref[...].astype(jnp.float32),
            (((1,), (1,)), ((), ())),
            precision=HIGHEST,
            preferred_element_type=jnp.float32,
        )
        source = [source_ref[i].astype(jnp.float32) for i in range(3)]

        load_plan.wait()
        sink = sink_ref[0]
        width = 1 + 2 * trees + directions

        def pick(candidate, chosen):
            return tuple(
                jnp.where(sink == candidate, plan_ref[0, candidate * width + q], chosen[q])
                for q in range(width)
            )

        plan = lax.fori_loop(0, grid.nodes, pick, (jnp.int32(-1),) * width)
        everywhere = [jnp.full((SUB, LANES), value, jnp.int32) for value in plan]
        is_source = everywhere[0] == 1
        parents = everywhere[1 : 1 + trees]
        depths = everywhere[1 + trees : 1 + 2 * trees]
        loads = everywhere[1 + 2 * trees :]

        def run(unit, start, stop):
            lax.fori_loop(start, stop, lambda u, carry: (unit(u), carry)[1], 0)

        def take(field, part, row, column, block):
            sites = pl.ds(pl.multiple_of(block * (SUB * LANES), SUB * LANES), SUB * LANES)
            return field[part, row, column, :, sites].reshape(SUB, LANES)

        def first_pair(row):
            return row * SPINCOLOR - lax.div(row * (row - 1), 2)

        def sigma_unit(unit):
            block, r = lax.div(unit, sigma_units), lax.rem(unit, sigma_units)
            last = SPINCOLOR - 1 - r
            upper, lower = first_pair(r) + block * len(PAIRS), first_pair(last) + block * len(PAIRS)
            for i in range(SPINCOLOR + 1):
                first = i < SPINCOLOR - r
                row = jnp.where(first, r, last)
                column = jnp.where(first, r + i, i - 1)
                total = None
                for m in range(SPINCOLOR):
                    left = [take(s_ref, part, row, m, block) for part in range(2)]
                    right = [take(s_ref, part, column, m, block) for part in range(2)]
                    total = multiply_add(total, left, right)
                number = jnp.where(first, upper + i, lower + i - 1 - last)
                place = pl.multiple_of(number * (2 * SUB), SUB)
                own_ref[pl.ds(place, SUB)] = 0.125 * total[0]
                own_ref[pl.ds(place + SUB, SUB)] = 0.125 * total[1]

        def sum_unit(unit):
            row, column = lax.div(unit, SPINCOLOR), lax.rem(unit, SPINCOLOR)
            for i in range(blocks):
                start = pl.multiple_of((unit * blocks + i) * SUB, SUB)
                hs_ref[pl.ds(start, SUB)] = take(h_ref, 0, row, column, i) + take(
                    h_ref, 1, row, column, i
                )

        def phase_row(number):
            lane = lax.broadcasted_iota(jnp.int32, (1, LANES), 1)
            site = (core * (rows * LANES) + number * LANES + lane).astype(jnp.float32)
            zplane = jnp.floor((site + 0.5) * (1.0 / (L * L)))
            rest = site - zplane * (L * L)
            xline = jnp.floor((rest + 0.5) * (1.0 / L))
            yline = rest - xline * L
            wave = (
                momenta[:, 0:1] * (xline - source[0])
                + momenta[:, 1:2] * (yline - source[1])
                + momenta[:, 2:3] * (zplane - source[2])
            )
            wave = wave - L * jnp.floor((wave + 0.5) * (1.0 / L)) - L / 2
            x = wave * (math.pi / L)
            y = x * x
            s = x * (1 + y * (-1 / 6 + y * (1 / 120 + y * (-1 / 5040 + y * (1 / 362880 - y / 39916800)))))
            c = 1 + y * (
                -1 / 2
                + y * (1 / 24 + y * (-1 / 720 + y * (1 / 40320 + y * (-1 / 3628800 + y / 479001600))))
            )
            inside = jnp.where(number < rows, 1.0, 0.0)
            block = lax.div(number, SUB)
            lanes = pl.ds(pl.multiple_of(lax.rem(number, SUB) * LANES, LANES), LANES)
            phase_ref[block, 0:padded, lanes] = (2.0 * s * s - 1.0) * inside
            phase_ref[block, padded : 2 * padded, lanes] = (2.0 * s * c) * inside

        def spin_unit(unit):
            block, k = lax.div(unit, spin_units), lax.rem(unit, spin_units)
            own_row = first_pair(k) - k
            column = []
            for m in range(SPINCOLOR):
                number = jnp.where(k >= m, PAIR_NUMBER[m, m] - m + k, own_row + m)
                place = pl.multiple_of((block * len(PAIRS) + number) * (2 * SUB), SUB)
                real, imag = tree_ref[pl.ds(place, SUB)], tree_ref[pl.ds(place + SUB, SUB)]
                column.append((real, imag - real, imag + real))
            for alpha in range(4):
                sums = [None] * 4
                for color in range(3):
                    parts = [None] * 3
                    for m in range(SPINCOLOR):
                        row = alpha * 3 + color
                        start = pl.multiple_of(
                            ((row * SPINCOLOR + m) * blocks + block) * SUB, SUB
                        )
                        back = (
                            hs_ref[pl.ds(start, SUB)],
                            take(h_ref, 0, row, m, block),
                            take(h_ref, 1, row, m, block),
                        )
                        for n in range(3):
                            term = back[n] * column[m][n]
                            parts[n] = term if parts[n] is None else parts[n] + term
                    total = (parts[0] - parts[2], parts[0] + parts[1])
                    for beta in range(4):
                        forward = [take(s_ref, part, beta * 3 + color, k, block) for part in range(2)]
                        sums[beta] = multiply_add_conj(sums[beta], forward, total)
                for beta in range(4):
                    for part in range(2):
                        place = pl.ds((part * 16 + beta * 4 + alpha) * SUB, SUB)
                        m_ref[place] = sums[beta][part] + jnp.where(k > 0, m_ref[place], 0.0)

            @pl.when(k == spin_units - 1)
            def _():
                spin = jnp.concatenate(
                    [m_ref[pl.ds(i, 32, stride=SUB), :] for i in range(SUB)], axis=1
                )
                acc_ref[...] += lax.dot_general(
                    spin,
                    phase_ref[block],
                    (((1,), (1,)), ((), ())),
                    precision=HIGHEST,
                    preferred_element_type=jnp.float32,
                )

        def out_copy(d, slot):
            place = lax.rem(slot, ring)
            return pltpu.make_async_remote_copy(
                src_ref=stage_ref.at[d, place],
                dst_ref=in_ref.at[d, place],
                send_sem=send_sem.at[d, place],
                recv_sem=recv_sem.at[d, place],
                device_id={"ta": neighbours[d]},
                device_id_type=MESH,
            )

        def settle(chunk):
            for k in range(trees):
                at_depth = [depths[k] == n for n in range(deepest + 1)]
                for i in range(piece):
                    value = None
                    for n in range(deepest + 1):
                        start = (chunk + hop * n) * all_rows + (i * trees + k) * SUB
                        found = a_ref[pl.ds(pl.multiple_of(start, SUB), SUB)]
                        value = found if value is None else jnp.where(at_depth[n], found, value)
                    start = chunk * all_rows + (i * trees + k) * SUB
                    tree_ref[pl.ds(pl.multiple_of(start, SUB), SUB)] = value

        def relay(j):
            @pl.when(j >= hop)
            def _():
                for d in range(directions):
                    when(has_in[d], lambda d=d: out_copy(d, j + ring - hop).wait_recv())

            @pl.when(jnp.logical_and(j >= ring, j < sends + ring))
            def _():
                for d in range(directions):
                    when(has_out[d], lambda d=d: out_copy(d, j).wait_send())

            place = lax.rem(j, ring)
            from_place = lax.rem(j + ring - hop, ring)
            mine = jnp.minimum(j, slots - 1) * all_rows
            for i in range(piece):
                at = slice(i * SUB, (i + 1) * SUB)
                arrived = [in_ref[d, from_place, at] for d in range(directions)]
                values = []
                for k in range(trees):
                    value = arrived[0]
                    for d in range(1, directions):
                        value = jnp.where(parents[k] == d, arrived[d], value)
                    offset = (i * trees + k) * SUB
                    start = pl.multiple_of(mine + offset, SUB)
                    value = jnp.where(is_source, own_ref[pl.ds(start, SUB)], value)
                    a_ref[pl.ds(pl.multiple_of(j * all_rows + offset, SUB), SUB)] = value
                    values.append(value)
                for d in range(directions):
                    value = values[0]
                    for k in range(1, trees):
                        value = jnp.where(loads[d] == k, values[k], value)
                    stage_ref[d, place, at] = value

            @pl.when(j >= hop * deepest)
            def _():
                settle(j - hop * deepest)

            @pl.when(j < sends)
            def _():
                for d in range(directions):
                    when(has_out[d], lambda d=d: out_copy(d, j).start())

        load_s.wait()
        load_h.start()
        run(sigma_unit, 0, sigma_units)

        peers = 1
        for known in has_in:
            peers += 1 if known is None else known.astype(jnp.int32)
        pl.semaphore_wait(barrier, peers)

        def sigma_until(j):
            done = sigma_units + (3 * sigma_units * (piece * (j + 2)) + 2 * share - 1) // (2 * share)
            return jnp.where(j < 0, sigma_units, jnp.minimum(done, sigma_units * blocks))

        phase_count = blocks * SUB

        sum_first, sum_last = 8, hop * deepest - 1
        sum_total = SPINCOLOR * SPINCOLOR

        def sum_until(j):
            done = lax.div((j + 1 - sum_first) * sum_total, sum_last - sum_first)
            return jnp.where(j < sum_first, 0, jnp.minimum(done, sum_total))

        spin_total = spin_units * blocks

        def spin_until(j):
            there = j - hop * deepest + 1
            done = (there * (100 * spin_units * piece) // share + 100 - behind) // 100
            return jnp.where(there <= 0, 0, jnp.clip(done, 0, spin_total))

        def step(j, carry):
            relay(j)
            run(sigma_unit, sigma_until(j - 1), sigma_until(j))
            run(
                phase_row,
                jnp.minimum(2 * j, phase_count),
                jnp.minimum(2 * j + 2, phase_count),
            )

            @pl.when(j == sum_first)
            def _():
                load_h.wait()

            run(sum_unit, sum_until(j - 1), sum_until(j))
            run(spin_unit, spin_until(j - 1), spin_until(j))
            return carry

        lax.fori_loop(0, all_slots, step, 0)
        run(spin_unit, spin_until(all_slots - 1), spin_total)

        def sent(slot):
            for d in range(directions):
                when(has_out[d], lambda d=d: out_copy(d, slot).wait_send())

        run(sent, all_slots - ring, sends)

        real = acc_ref[0:16, 0:padded] - acc_ref[16:32, padded : 2 * padded]
        imag = acc_ref[0:16, padded : 2 * padded] + acc_ref[16:32, 0:padded]
        send_ref[0:16, 0:padded] = real
        send_ref[16:32, 0:padded] = imag
        swap = pltpu.make_async_remote_copy(
            src_ref=send_ref,
            dst_ref=got_ref,
            send_sem=pair_sem.at[0],
            recv_sem=pair_sem.at[1],
            device_id={"gz": partner},
            device_id_type=MESH,
        )
        swap.start()
        swap.wait()
        both = send_ref[:, 0:padded] + got_ref[:, 0:padded]
        result = lax.dot_general(
            w_ref[...],
            both,
            (((1,), (0,)), ((), ())),
            precision=HIGHEST,
            preferred_element_type=jnp.float32,
        )
        out_ref[0, 0] = result[0:currents, 0:momentum_count]
        out_ref[1, 0] = result[currents : 2 * currents, 0:momentum_count]

    scratch = [
        pltpu.VMEM((2, SPINCOLOR, SPINCOLOR, 1, blocks * SUB * LANES), jnp.float32),
        pltpu.VMEM((2, SPINCOLOR, SPINCOLOR, 1, blocks * SUB * LANES), jnp.float32),
        pltpu.VMEM((SPINCOLOR * SPINCOLOR * blocks * SUB, LANES), jnp.float32),
        pltpu.VMEM((slots * all_rows, LANES), jnp.float32),
        pltpu.VMEM(((slots + most_hop * deepest) * all_rows, LANES), jnp.float32),
        pltpu.VMEM((slots * all_rows, LANES), jnp.float32),
        pltpu.VMEM((directions, ring, piece_rows, LANES), jnp.float32),
        pltpu.VMEM((directions, ring, piece_rows, LANES), jnp.float32),
        pltpu.VMEM((blocks, 2 * padded, SUB * LANES), jnp.float32),
        pltpu.VMEM((32 * SUB, LANES), jnp.float32),
        pltpu.VMEM((32, 2 * padded), jnp.float32),
        pltpu.VMEM((2 * currents, 32), jnp.float32),
        pltpu.VMEM((32, LANES), jnp.float32),
        pltpu.VMEM((32, LANES), jnp.float32),
        pltpu.SMEM((1, plan_width(grid, trees)), jnp.int32),
        pltpu.SemaphoreType.DMA((2,)),
        pltpu.SemaphoreType.DMA(()),
        pltpu.SemaphoreType.DMA((directions, ring)),
        pltpu.SemaphoreType.DMA((directions, ring)),
        pltpu.SemaphoreType.DMA((2,)),
    ]
    return kernel, scratch


def plan_width(grid, trees):
    used = grid.nodes * (1 + 2 * trees + len(grid.dirs))
    return pl.cdiv(used, LANES) * LANES


def mixing():
    real, imag = np.transpose(gamma_tables(), (0, 1, 3, 2)).reshape(2, 16, 16)
    scale = 1.0 / (72.0 * math.sqrt(L * L * L))
    return (
        scale
        * np.stack([np.concatenate([real, -imag], axis=1), np.concatenate([imag, real], axis=1)])
    ).astype(np.float32)


def solution(mesh):
    grid = Grid(mesh)
    trees, deepest, table = routes(grid)
    cores = mesh.shape["gz"]
    width = plan_width(grid, trees)
    flat = table.reshape(grid.nodes, -1)
    plans = np.zeros((grid.nodes, 1, width), np.int32)
    plans[:, 0, : flat.shape[1]] = flat
    mix = mixing()

    def body(propagator, backward, sink_time, source_position, momenta, gamma_table):
        local_times, site_count = propagator.shape[3:]
        assert local_times == 1 and cores == 2 and site_count % LANES == 0
        rows = site_count // LANES
        momentum_count = momenta.shape[0]
        currents = gamma_table.shape[0] // cores
        kernel, scratch = make_kernel(grid, trees, deepest, rows, momentum_count, currents)
        vmem, smem = (
            pl.BlockSpec(memory_space=pltpu.VMEM),
            pl.BlockSpec(memory_space=pltpu.SMEM),
        )
        anywhere = pl.BlockSpec(memory_space=pl.ANY)
        return pl.pallas_call(
            kernel,
            out_shape=jax.ShapeDtypeStruct((2, 1, currents, momentum_count), jnp.float32),
            in_specs=[smem, smem, smem, vmem, vmem, anywhere, anywhere, anywhere],
            out_specs=vmem,
            scratch_shapes=scratch,
            compiler_params=pltpu.CompilerParams(
                collective_id=0, has_side_effects=True, vmem_limit_bytes=60 << 20
            ),
            name="three_point",
        )(
            sink_time,
            source_position,
            gamma_table,
            momenta.T,
            jnp.asarray(mix),
            jnp.asarray(plans),
            propagator,
            backward,
        )

    in_specs = (
        P(None, None, None, "ta", "gz"),
        P(None, None, None, "ta", "gz"),
        P(),
        P(),
        P(),
        P(),
    )
    out_specs = P(None, "ta", "gz", None)
    return jax.shard_map(body, mesh=mesh, in_specs=in_specs, out_specs=out_specs, check_vma=False)
```

```python
import math
import random

import jax
import jax.numpy as jnp
import numpy as np
from jax import lax
from jax.experimental import pallas as pl
from jax.experimental.pallas import tpu as pltpu
from jax.sharding import PartitionSpec as P

L = 24
NG = 16
LANES = 128
SUB = 8
SPINCOLOR = 12
PAIRS = [(row, column) for row in range(SPINCOLOR) for column in range(row, SPINCOLOR)]
PAIR_NUMBER = {pair: number for number, pair in enumerate(PAIRS)}
HOP_SLOTS = (5, 4)
PIECE = 7
MESH = pl.DeviceIdType.MESH
HIGHEST = lax.Precision.HIGHEST


def gamma_tables():
    paulis = [
        np.eye(2),
        np.array([[0.0, 1.0], [1.0, 0.0]]),
        np.array([[0.0, -1j], [1j, 0.0]]),
        np.array([[1.0, 0.0], [0.0, -1.0]]),
    ]
    matrices = np.stack([np.kron(paulis[number // 4], paulis[number % 4]) for number in range(16)])
    return np.stack([matrices.real, matrices.imag]).astype(np.float32)


class Grid:
    def __init__(self, mesh):
        devices = mesh.devices.reshape(mesh.shape["ta"], -1)[:, 0]
        self.nodes = len(devices)
        self.dims, self.strides, self.wrap = [self.nodes], [1], False
        coords = [getattr(device, "coords", None) for device in devices]
        if all(coord is not None for coord in coords):
            self.read(np.array([list(coord) for coord in coords]))
        self.dirs = []
        for axis, size in enumerate(self.dims):
            if size == 2:
                self.dirs.append((axis, 0))
            elif size > 2:
                self.dirs += [(axis, 1), (axis, -1)]

    def read(self, coords):
        coords = coords - coords.min(axis=0)
        sizes = coords.max(axis=0) + 1
        found = []
        for axis in range(coords.shape[1]):
            if sizes[axis] > 1:
                unit = np.zeros(coords.shape[1], int)
                unit[axis] = 1
                hits = np.flatnonzero((coords == unit).all(axis=1))
                if len(hits) != 1:
                    return
                found.append((int(hits[0]), int(sizes[axis]), axis))
        found.sort(reverse=True)
        index = np.arange(self.nodes)
        for stride, size, axis in found:
            if ((index // stride) % size != coords[:, axis]).any():
                return
        if math.prod(size for _, size, _ in found) != self.nodes:
            return
        self.dims = [size for _, size, _ in found]
        self.strides = [stride for stride, _, _ in found]
        self.wrap = len(found) == 3 and all(size % 4 == 0 for size in self.dims)

    def position(self, node):
        return [node // stride % size for stride, size in zip(self.strides, self.dims)]

    def node(self, position):
        return sum(c * stride for c, stride in zip(position, self.strides))

    def step(self, node, number):
        axis, sign = self.dirs[number]
        place = self.position(node)
        place[axis] = 1 - place[axis] if sign == 0 else place[axis] + sign
        if self.wrap:
            place[axis] %= self.dims[axis]
        if not 0 <= place[axis] < self.dims[axis]:
            return None
        return self.node(place)


def grow(edges, nodes, root, count, rng, deepest):
    used = set()
    depth = [{root: 0} for _ in range(count)]
    parent = [{} for _ in range(count)]
    from_root = [0] * count
    for _ in range(deepest):
        options = [
            (k, u, d, v)
            for k in range(count)
            for u in depth[k]
            for d, v in edges[u]
            if v not in depth[k] and (u, d) not in used
        ]
        rng.shuffle(options)
        ways = {}
        for k, _, _, v in options:
            ways[k, v] = ways.get((k, v), 0) + 1
        options.sort(key=lambda option: ways[option[0], option[3]] + 1.5 * rng.random())
        level = [{} for _ in range(count)]
        taken = [0] * count
        for k, u, d, v in options:
            if v in depth[k] or v in level[k] or (u, d) in used:
                continue
            if u == root:
                if taken[k] or (from_root[k] and rng.random() < 0.7):
                    continue
                taken[k] = 1
                from_root[k] += 1
            level[k][v] = depth[k][u] + 1
            parent[k][v] = (u, d)
            used.add((u, d))
        for k in range(count):
            depth[k].update(level[k])
        if all(len(known) == nodes for known in depth):
            return sorted(max(known.values()) for known in depth)[::-1], parent, depth
    return None


def route(grid, root):
    edges = {
        u: [
            (d, v)
            for d in range(len(grid.dirs))
            for v in [grid.step(u, d)]
            if v is not None and v != u
        ]
        for u in range(grid.nodes)
    }
    rng = random.Random(7)
    most = min(3, min(len(links) for links in edges.values()))
    for count in range(most, 0, -1):
        best = None
        for _ in range(400 if grid.nodes <= 16 else 40):
            found = grow(edges, grid.nodes, root, count, rng, 2 * sum(grid.dims))
            if found and (best is None or found[0] < best[0]):
                best = found
        if best:
            return count, best[1], best[2]
    raise ValueError("no route")


def routes(grid):
    plans = {}
    for root in range(grid.nodes):
        place = grid.position(root)
        if grid.wrap:
            canonical = 0
        else:
            canonical = grid.node([min(c, n - 1 - c) for c, n in zip(place, grid.dims)])
        if canonical not in plans:
            plans[canonical] = route(grid, canonical)
    trees = min(plan[0] for plan in plans.values())
    width = 1 + 2 * trees + len(grid.dirs)
    table = np.full((grid.nodes, grid.nodes, width), -1, np.int32)
    deepest = 0
    for root in range(grid.nodes):
        place = grid.position(root)
        if grid.wrap:
            canonical, flips = 0, [False] * len(place)
        else:
            flips = [c > n - 1 - c for c, n in zip(place, grid.dims)]
            canonical = grid.node([min(c, n - 1 - c) for c, n in zip(place, grid.dims)])

        def image(node):
            there = grid.position(node)
            if grid.wrap:
                return grid.node([(c + o) % n for c, o, n in zip(there, place, grid.dims)])
            return grid.node([n - 1 - c if f else c for c, f, n in zip(there, flips, grid.dims)])

        def turned(d):
            axis, sign = grid.dirs[d]
            return grid.dirs.index((axis, -sign if flips[axis] else sign))

        _, parent, depth = plans[canonical]
        for k in range(trees):
            for v in range(grid.nodes):
                row = table[image(v), root]
                row[0] = v == canonical
                row[1 + trees + k] = depth[k][v]
                deepest = max(deepest, depth[k][v])
                if v != canonical:
                    u, d = parent[k][v]
                    row[1 + k] = turned(d)
                    sender = table[image(u), root]
                    assert sender[1 + 2 * trees + turned(d)] == -1
                    sender[1 + 2 * trees + turned(d)] = k
    return trees, deepest, table


def multiply_add(total, left, right):
    real = left[0] * right[0] - left[1] * right[1]
    imag = left[0] * right[1] + left[1] * right[0]
    return (real, imag) if total is None else (total[0] + real, total[1] + imag)


def multiply_add_conj(total, left, right):
    real = left[0] * right[0] + left[1] * right[1]
    imag = left[1] * right[0] - left[0] * right[1]
    return (real, imag) if total is None else (total[0] + real, total[1] + imag)


def make_kernel(grid, trees, deepest, rows, momentum_count, currents):
    blocks = pl.cdiv(rows, SUB)
    share = 2 * len(PAIRS) // trees
    piece = PIECE if share * blocks % PIECE == 0 else blocks
    slots = share * blocks // piece
    most_hop = max(HOP_SLOTS)
    ring = 2 * most_hop
    directions = len(grid.dirs)
    sigma_units = 6
    spin_units = SPINCOLOR
    piece_rows = piece * SUB
    all_rows = trees * piece_rows
    ready = [
        ((2 * PAIR_NUMBER[k, SPINCOLOR - 1] + 1) // trees + 1) / share for k in range(SPINCOLOR)
    ]
    behind = math.ceil(100 * max(spin_units * ready[k] - k for k in range(SPINCOLOR)))
    padded = 32

    def kernel(
        sink_ref, source_ref, gamma_ref, momenta_ref, mix_ref, table_ref, s_hbm, h_hbm,
        out_ref,
        s_ref, h_ref, hs_ref, own_ref, a_ref, tree_ref, in_ref, stage_ref, phase_ref,
        m_ref, acc_ref, w_ref, send_ref, got_ref, plan_ref,
        load_sem, plan_sem, send_sem, recv_sem, pair_sem,
    ):
        me = lax.axis_index("ta")
        core = lax.axis_index("gz")
        partner = 1 - core
        hop = jnp.where(core == 1, HOP_SLOTS[1], HOP_SLOTS[0])
        all_slots = slots + hop * deepest
        sends = all_slots - hop
        inside = pl.ds(0, rows * LANES)
        load_s = pltpu.make_async_copy(s_hbm, s_ref.at[:, :, :, :, inside], load_sem.at[0])
        load_h = pltpu.make_async_copy(h_hbm, h_ref.at[:, :, :, :, inside], load_sem.at[1])
        load_s.start()
        load_plan = pltpu.make_async_copy(table_ref.at[me], plan_ref, plan_sem)
        load_plan.start()

        neighbours, has_out, has_in = [], [], []
        for axis, sign in grid.dirs:
            stride, size = grid.strides[axis], grid.dims[axis]
            place = me // stride % size
            if sign == 0:
                neighbours.append(me + stride * (1 - 2 * place))
                has_out.append(None)
                has_in.append(None)
            elif grid.wrap:
                neighbours.append(me + stride * ((place + sign + size) % size - place))
                has_out.append(None)
                has_in.append(None)
            else:
                neighbours.append(me + stride * sign)
                has_out.append(place < size - 1 if sign > 0 else place > 0)
                has_in.append(place > 0 if sign > 0 else place < size - 1)

        def when(condition, action):
            if condition is None:
                action()
            else:
                pl.when(condition)(action)

        barrier = pltpu.get_barrier_semaphore()
        pl.semaphore_signal(barrier, 1, device_id={"gz": partner}, device_id_type=MESH)
        for d in range(directions):

            def greet(d=d):
                pl.semaphore_signal(
                    barrier, 1, device_id={"ta": neighbours[d]}, device_id_type=MESH
                )

            when(has_out[d], greet)

        acc_ref[...] = jnp.zeros_like(acc_ref)
        spare = (blocks * SUB - rows) * LANES
        if spare:
            for field in (s_ref, h_ref):
                for part in range(2):
                    for row in range(SPINCOLOR):
                        field[part, row, :, :, pl.ds(rows * LANES, spare)] = jnp.zeros(
                            (SPINCOLOR, 1, spare), jnp.float32
                        )
        names = lax.broadcasted_iota(jnp.int32, (1, NG), 1)
        onehot = jnp.concatenate(
            [
                jnp.where(names == jnp.full((1, NG), gamma_ref[core * currents + c]), 1.0, 0.0)
                for c in range(currents)
            ],
            axis=0,
        )
        for part in range(2):
            w_ref[part * currents : (part + 1) * currents] = lax.dot_general(
                onehot,
                mix_ref[part],
                (((1,), (0,)), ((), ())),
                precision=HIGHEST,
                preferred_element_type=jnp.float32,
            )
        eye = jnp.where(
            lax.broadcasted_iota(jnp.int32, (padded, momentum_count), 0)
            == lax.broadcasted_iota(jnp.int32, (padded, momentum_count), 1),
            1.0,
            0.0,
        )
        momenta = lax.dot_general(
            eye,
            momenta_ref[...].astype(jnp.float32),
            (((1,), (1,)), ((), ())),
            precision=HIGHEST,
            preferred_element_type=jnp.float32,
        )
        source = [source_ref[i].astype(jnp.float32) for i in range(3)]

        load_plan.wait()
        sink = sink_ref[0]
        width = 1 + 2 * trees + directions

        def pick(candidate, chosen):
            return tuple(
                jnp.where(sink == candidate, plan_ref[0, candidate * width + q], chosen[q])
                for q in range(width)
            )

        plan = lax.fori_loop(0, grid.nodes, pick, (jnp.int32(-1),) * width)
        everywhere = [jnp.full((SUB, LANES), value, jnp.int32) for value in plan]
        is_source = everywhere[0] == 1
        parents = everywhere[1 : 1 + trees]
        depths = everywhere[1 + trees : 1 + 2 * trees]
        loads = everywhere[1 + 2 * trees :]

        def run(unit, start, stop):
            lax.fori_loop(start, stop, lambda u, carry: (unit(u), carry)[1], 0)

        def take(field, part, row, column, block):
            sites = pl.ds(pl.multiple_of(block * (SUB * LANES), SUB * LANES), SUB * LANES)
            return field[part, row, column, :, sites].reshape(SUB, LANES)

        def first_pair(row):
            return row * SPINCOLOR - lax.div(row * (row - 1), 2)

        def sigma_unit(unit):
            block, r = lax.div(unit, sigma_units), lax.rem(unit, sigma_units)
            last = SPINCOLOR - 1 - r
            upper, lower = first_pair(r) + block * len(PAIRS), first_pair(last) + block * len(PAIRS)
            for i in range(SPINCOLOR + 1):
                first = i < SPINCOLOR - r
                row = jnp.where(first, r, last)
                column = jnp.where(first, r + i, i - 1)
                total = None
                for m in range(SPINCOLOR):
                    left = [take(s_ref, part, row, m, block) for part in range(2)]
                    right = [take(s_ref, part, column, m, block) for part in range(2)]
                    total = multiply_add(total, left, right)
                number = jnp.where(first, upper + i, lower + i - 1 - last)
                place = pl.multiple_of(number * (2 * SUB), SUB)
                own_ref[pl.ds(place, SUB)] = 0.125 * total[0]
                own_ref[pl.ds(place + SUB, SUB)] = 0.125 * total[1]

        def sum_unit(unit):
            row, column = lax.div(unit, SPINCOLOR), lax.rem(unit, SPINCOLOR)
            for i in range(blocks):
                start = pl.multiple_of((unit * blocks + i) * SUB, SUB)
                hs_ref[pl.ds(start, SUB)] = take(h_ref, 0, row, column, i) + take(
                    h_ref, 1, row, column, i
                )

        def phase_row(number):
            lane = lax.broadcasted_iota(jnp.int32, (1, LANES), 1)
            site = (core * (rows * LANES) + number * LANES + lane).astype(jnp.float32)
            zplane = jnp.floor((site + 0.5) * (1.0 / (L * L)))
            rest = site - zplane * (L * L)
            xline = jnp.floor((rest + 0.5) * (1.0 / L))
            yline = rest - xline * L
            wave = (
                momenta[:, 0:1] * (xline - source[0])
                + momenta[:, 1:2] * (yline - source[1])
                + momenta[:, 2:3] * (zplane - source[2])
            )
            wave = wave - L * jnp.floor((wave + 0.5) * (1.0 / L)) - L / 2
            x = wave * (math.pi / L)
            y = x * x
            s = x * (1 + y * (-1 / 6 + y * (1 / 120 + y * (-1 / 5040 + y * (1 / 362880 - y / 39916800)))))
            c = 1 + y * (
                -1 / 2
                + y * (1 / 24 + y * (-1 / 720 + y * (1 / 40320 + y * (-1 / 3628800 + y / 479001600))))
            )
            inside = jnp.where(number < rows, 1.0, 0.0)
            block = lax.div(number, SUB)
            lanes = pl.ds(pl.multiple_of(lax.rem(number, SUB) * LANES, LANES), LANES)
            phase_ref[block, 0:padded, lanes] = (2.0 * s * s - 1.0) * inside
            phase_ref[block, padded : 2 * padded, lanes] = (2.0 * s * c) * inside

        def spin_unit(unit):
            block, k = lax.div(unit, spin_units), lax.rem(unit, spin_units)
            own_row = first_pair(k) - k
            column = []
            for m in range(SPINCOLOR):
                number = jnp.where(k >= m, PAIR_NUMBER[m, m] - m + k, own_row + m)
                place = pl.multiple_of((block * len(PAIRS) + number) * (2 * SUB), SUB)
                real, imag = tree_ref[pl.ds(place, SUB)], tree_ref[pl.ds(place + SUB, SUB)]
                column.append((real, imag - real, imag + real))
            for alpha in range(4):
                sums = [None] * 4
                for color in range(3):
                    parts = [None] * 3
                    for m in range(SPINCOLOR):
                        row = alpha * 3 + color
                        start = pl.multiple_of(
                            ((row * SPINCOLOR + m) * blocks + block) * SUB, SUB
                        )
                        back = (
                            hs_ref[pl.ds(start, SUB)],
                            take(h_ref, 0, row, m, block),
                            take(h_ref, 1, row, m, block),
                        )
                        for n in range(3):
                            term = back[n] * column[m][n]
                            parts[n] = term if parts[n] is None else parts[n] + term
                    total = (parts[0] - parts[2], parts[0] + parts[1])
                    for beta in range(4):
                        forward = [take(s_ref, part, beta * 3 + color, k, block) for part in range(2)]
                        sums[beta] = multiply_add_conj(sums[beta], forward, total)
                for beta in range(4):
                    for part in range(2):
                        place = pl.ds((part * 16 + beta * 4 + alpha) * SUB, SUB)
                        m_ref[place] = sums[beta][part] + jnp.where(k > 0, m_ref[place], 0.0)

            @pl.when(k == spin_units - 1)
            def _():
                spin = jnp.concatenate(
                    [m_ref[pl.ds(i, 32, stride=SUB), :] for i in range(SUB)], axis=1
                )
                acc_ref[...] += lax.dot_general(
                    spin,
                    phase_ref[block],
                    (((1,), (1,)), ((), ())),
                    precision=HIGHEST,
                    preferred_element_type=jnp.float32,
                )

        def out_copy(d, slot):
            place = lax.rem(slot, ring)
            return pltpu.make_async_remote_copy(
                src_ref=stage_ref.at[d, place],
                dst_ref=in_ref.at[d, place],
                send_sem=send_sem.at[d, place],
                recv_sem=recv_sem.at[d, place],
                device_id={"ta": neighbours[d]},
                device_id_type=MESH,
            )

        def settle(chunk):
            for k in range(trees):
                at_depth = [depths[k] == n for n in range(deepest + 1)]
                for i in range(piece):
                    value = None
                    for n in range(deepest + 1):
                        start = (chunk + hop * n) * all_rows + (i * trees + k) * SUB
                        found = a_ref[pl.ds(pl.multiple_of(start, SUB), SUB)]
                        value = found if value is None else jnp.where(at_depth[n], found, value)
                    start = chunk * all_rows + (i * trees + k) * SUB
                    tree_ref[pl.ds(pl.multiple_of(start, SUB), SUB)] = value

        def relay(j):
            @pl.when(j >= hop)
            def _():
                for d in range(directions):
                    when(has_in[d], lambda d=d: out_copy(d, j + ring - hop).wait_recv())

            @pl.when(jnp.logical_and(j >= ring, j < sends + ring))
            def _():
                for d in range(directions):
                    when(has_out[d], lambda d=d: out_copy(d, j).wait_send())

            place = lax.rem(j, ring)
            from_place = lax.rem(j + ring - hop, ring)
            mine = jnp.minimum(j, slots - 1) * all_rows
            for i in range(piece):
                at = slice(i * SUB, (i + 1) * SUB)
                arrived = [in_ref[d, from_place, at] for d in range(directions)]
                values = []
                for k in range(trees):
                    value = arrived[0]
                    for d in range(1, directions):
                        value = jnp.where(parents[k] == d, arrived[d], value)
                    offset = (i * trees + k) * SUB
                    start = pl.multiple_of(mine + offset, SUB)
                    value = jnp.where(is_source, own_ref[pl.ds(start, SUB)], value)
                    a_ref[pl.ds(pl.multiple_of(j * all_rows + offset, SUB), SUB)] = value
                    values.append(value)
                for d in range(directions):
                    value = values[0]
                    for k in range(1, trees):
                        value = jnp.where(loads[d] == k, values[k], value)
                    stage_ref[d, place, at] = value

            @pl.when(j >= hop * deepest)
            def _():
                settle(j - hop * deepest)

            @pl.when(j < sends)
            def _():
                for d in range(directions):
                    when(has_out[d], lambda d=d: out_copy(d, j).start())

        load_s.wait()
        load_h.start()
        run(sigma_unit, 0, sigma_units)

        peers = 1
        for known in has_in:
            peers += 1 if known is None else known.astype(jnp.int32)
        pl.semaphore_wait(barrier, peers)

        def sigma_until(j):
            done = sigma_units + (3 * sigma_units * (piece * (j + 2)) + 2 * share - 1) // (2 * share)
            return jnp.where(j < 0, sigma_units, jnp.minimum(done, sigma_units * blocks))

        phase_count = blocks * SUB

        sum_first, sum_last = 8, hop * deepest - 1
        sum_total = SPINCOLOR * SPINCOLOR

        def sum_until(j):
            done = lax.div((j + 1 - sum_first) * sum_total, sum_last - sum_first)
            return jnp.where(j < sum_first, 0, jnp.minimum(done, sum_total))

        spin_total = spin_units * blocks

        def spin_until(j):
            there = j - hop * deepest + 1
            done = (there * (100 * spin_units * piece) // share + 100 - behind) // 100
            return jnp.where(there <= 0, 0, jnp.clip(done, 0, spin_total))

        def step(j, carry):
            relay(j)
            run(sigma_unit, sigma_until(j - 1), sigma_until(j))
            run(
                phase_row,
                jnp.minimum(2 * j, phase_count),
                jnp.minimum(2 * j + 2, phase_count),
            )

            @pl.when(j == sum_first)
            def _():
                load_h.wait()

            run(sum_unit, sum_until(j - 1), sum_until(j))
            run(spin_unit, spin_until(j - 1), spin_until(j))
            return carry

        lax.fori_loop(0, all_slots, step, 0)
        run(spin_unit, spin_until(all_slots - 1), spin_total)

        def sent(slot):
            for d in range(directions):
                when(has_out[d], lambda d=d: out_copy(d, slot).wait_send())

        run(sent, all_slots - ring, sends)

        real = acc_ref[0:16, 0:padded] - acc_ref[16:32, padded : 2 * padded]
        imag = acc_ref[0:16, padded : 2 * padded] + acc_ref[16:32, 0:padded]
        send_ref[0:16, 0:padded] = real
        send_ref[16:32, 0:padded] = imag
        swap = pltpu.make_async_remote_copy(
            src_ref=send_ref,
            dst_ref=got_ref,
            send_sem=pair_sem.at[0],
            recv_sem=pair_sem.at[1],
            device_id={"gz": partner},
            device_id_type=MESH,
        )
        swap.start()
        swap.wait()
        both = send_ref[:, 0:padded] + got_ref[:, 0:padded]
        result = lax.dot_general(
            w_ref[...],
            both,
            (((1,), (0,)), ((), ())),
            precision=HIGHEST,
            preferred_element_type=jnp.float32,
        )
        out_ref[0, 0] = result[0:currents, 0:momentum_count]
        out_ref[1, 0] = result[currents : 2 * currents, 0:momentum_count]

    scratch = [
        pltpu.VMEM((2, SPINCOLOR, SPINCOLOR, 1, blocks * SUB * LANES), jnp.float32),
        pltpu.VMEM((2, SPINCOLOR, SPINCOLOR, 1, blocks * SUB * LANES), jnp.float32),
        pltpu.VMEM((SPINCOLOR * SPINCOLOR * blocks * SUB, LANES), jnp.float32),
        pltpu.VMEM((slots * all_rows, LANES), jnp.float32),
        pltpu.VMEM(((slots + most_hop * deepest) * all_rows, LANES), jnp.float32),
        pltpu.VMEM((slots * all_rows, LANES), jnp.float32),
        pltpu.VMEM((directions, ring, piece_rows, LANES), jnp.float32),
        pltpu.VMEM((directions, ring, piece_rows, LANES), jnp.float32),
        pltpu.VMEM((blocks, 2 * padded, SUB * LANES), jnp.float32),
        pltpu.VMEM((32 * SUB, LANES), jnp.float32),
        pltpu.VMEM((32, 2 * padded), jnp.float32),
        pltpu.VMEM((2 * currents, 32), jnp.float32),
        pltpu.VMEM((32, LANES), jnp.float32),
        pltpu.VMEM((32, LANES), jnp.float32),
        pltpu.SMEM((1, plan_width(grid, trees)), jnp.int32),
        pltpu.SemaphoreType.DMA((2,)),
        pltpu.SemaphoreType.DMA(()),
        pltpu.SemaphoreType.DMA((directions, ring)),
        pltpu.SemaphoreType.DMA((directions, ring)),
        pltpu.SemaphoreType.DMA((2,)),
    ]
    return kernel, scratch


def plan_width(grid, trees):
    used = grid.nodes * (1 + 2 * trees + len(grid.dirs))
    return pl.cdiv(used, LANES) * LANES


def mixing():
    real, imag = np.transpose(gamma_tables(), (0, 1, 3, 2)).reshape(2, 16, 16)
    scale = 1.0 / (72.0 * math.sqrt(L * L * L))
    return (
        scale
        * np.stack([np.concatenate([real, -imag], axis=1), np.concatenate([imag, real], axis=1)])
    ).astype(np.float32)


def solution(mesh):
    grid = Grid(mesh)
    trees, deepest, table = routes(grid)
    cores = mesh.shape["gz"]
    width = plan_width(grid, trees)
    flat = table.reshape(grid.nodes, -1)
    plans = np.zeros((grid.nodes, 1, width), np.int32)
    plans[:, 0, : flat.shape[1]] = flat
    mix = mixing()

    def body(propagator, backward, sink_time, source_position, momenta, gamma_table):
        local_times, site_count = propagator.shape[3:]
        assert local_times == 1 and cores == 2 and site_count % LANES == 0
        rows = site_count // LANES
        momentum_count = momenta.shape[0]
        currents = gamma_table.shape[0] // cores
        kernel, scratch = make_kernel(grid, trees, deepest, rows, momentum_count, currents)
        vmem, smem = (
            pl.BlockSpec(memory_space=pltpu.VMEM),
            pl.BlockSpec(memory_space=pltpu.SMEM),
        )
        anywhere = pl.BlockSpec(memory_space=pl.ANY)
        return pl.pallas_call(
            kernel,
            out_shape=jax.ShapeDtypeStruct((2, 1, currents, momentum_count), jnp.float32),
            in_specs=[smem, smem, smem, vmem, vmem, anywhere, anywhere, anywhere],
            out_specs=vmem,
            scratch_shapes=scratch,
            compiler_params=pltpu.CompilerParams(
                collective_id=0, has_side_effects=True, vmem_limit_bytes=60 << 20
            ),
            name="three_point",
        )(
            sink_time,
            source_position,
            gamma_table,
            momenta.T,
            jnp.asarray(mix),
            jnp.asarray(plans),
            propagator,
            backward,
        )

    in_specs = (
        P(None, None, None, "ta", "gz"),
        P(None, None, None, "ta", "gz"),
        P(),
        P(),
        P(),
        P(),
    )
    out_specs = P(None, "ta", "gz", None)
    return jax.shard_map(body, mesh=mesh, in_specs=in_specs, out_specs=out_specs, check_vma=False)
```
